32 devices in a mesh: lat: 8 (over z, x), lev: 4 (over y, core).
Axes of the slice: x: 2, y: 2, z: 4, core: 2. Of those that a mesh axis runs over, the one named last changes fastest.
Arguments:
- right_side: float32 [8, 64, 2048], P('lev', 'lat'), may hold values from -6 to 6
- diag_shift: float32 [8, 64, 2048], P('lev', 'lat'), may hold values from 0.5 to 2
- level_scale: float32 [8], P('lev'), may hold values from 0.1 to 1
Outputs:
- solution: float32 [8, 64, 2048], P('lev', 'lat')
- residual: float32 [8, 64, 2048], P('lev', 'lat')
The draws below stay inside these ranges and needn't reach their ends.
All inputs are finite; a program needn't handle non-finite values.
Results may differ from the reference program's by a relative error of at most 0.0003.
Values sent between devices are 32-bit elements; how exact they have to be, the bound alone decides.
A program may use at most 64 MiB of HBM per device.

```python
import math
import jax
import jax.numpy as jnp
from jax import lax

NLON = 2048
WAVES = 640
ITERS = 3
NLAT = 64
LEVELS = 8


def block_scale(key, shape, cuts, low, top_value):
    loudness, own = 1.0, jax.random.fold_in(key, 6)
    for dim, parts in cuts:
        draws = jnp.exp(jax.random.uniform(jax.random.fold_in(own, dim), (parts,), jnp.float32, low / len(cuts), top_value / len(cuts)))
        loudness = loudness * jnp.repeat(draws, shape[dim] // parts).reshape([-1 if axis == dim else 1 for axis in range(len(shape))])
    return loudness


def noise(rng, shape, width, bound, pieces=(), held_as=jnp.bfloat16):
    result = jax.random.normal(rng, shape, jnp.float32) * width
    if len(pieces) > 0:
        result = block_scale(rng, shape, pieces, -0.22, 0.18) * result
    return jnp.clip(result, min=-bound, max=bound).astype(held_as)


def setup_inputs(seed: int = 0) -> dict:
    key_of = jax.random.split(jax.random.key(seed), 4)
    right_side = noise(key_of[0], (LEVELS, NLAT, NLON), 1.0, 6.0, ((0, 4), (1, 8)), jnp.float32)
    diag_shift = jnp.clip(0.5 + 1.5 * jax.random.uniform(key_of[1], (LEVELS, NLAT, NLON), jnp.float32) ** block_scale(key_of[1], (LEVELS, NLAT, NLON), ((0, 4), (1, 8)), -0.2, 0.2), 0.5, 2.0)
    level_scale = jnp.clip(jnp.exp(math.log(1.0) - 2.3025851 * jax.random.uniform(key_of[2], (LEVELS,), jnp.float32) ** block_scale(key_of[2], (LEVELS,), ((0, 4),), -0.2, 0.2)), 0.1, 1.0)
    return dict(right_side=right_side, diag_shift=diag_shift, level_scale=level_scale)


def polar_gain(total_rows, start, count):
    latitude = (start + jnp.arange(count, dtype=jnp.int32)).astype(jnp.float32)
    colatitude = jnp.pi * (4.0 * latitude + 3.0) / (4.0 * total_rows + 2.0)
    return 1.0 / jnp.maximum(jnp.sin(colatitude), 0.5) ** 2


def fourier_table(longitudes, wavenumber, cosine_part):
    position = jnp.arange(longitudes, dtype=jnp.int32)
    product = (position[:, None] * wavenumber[None, :]) % longitudes
    radians = (2.0 * jnp.pi / longitudes) * product.astype(jnp.float32)
    return jnp.where(cosine_part[None, :], jnp.cos(radians), jnp.sin(radians))


def sine_table(latitudes):
    counter = jnp.arange(1, latitudes + 1, dtype=jnp.int32)
    product = (counter[:, None] * counter[None, :]) % (2 * latitudes + 2)
    return jnp.sin((jnp.pi / (latitudes + 1)) * product.astype(jnp.float32))


def spectral_weights(latitudes, longitudes, wavenumber):
    counter = jnp.arange(1, latitudes + 1, dtype=jnp.int32).astype(jnp.float32)
    zonal_part = 4.0 * jnp.sin((jnp.pi / longitudes) * wavenumber.astype(jnp.float32)) ** 2
    merid_part = 4.0 * jnp.sin((0.5 * jnp.pi / (latitudes + 1)) * counter) ** 2
    scaling = 2.0 / (longitudes * (latitudes + 1))
    return scaling / (1.0 + merid_part[:, None] + zonal_part[None, :])


def stencil(padded, diagonal, level_scale, zonal_gain):
    centre = padded[:, 1:-1, :]
    meridional = padded[:, :-2, :] + padded[:, 2:, :]
    zonal_pair = jnp.roll(centre, 1, axis=2) + jnp.roll(centre, -1, axis=2)
    corners = jnp.roll(meridional, 1, axis=2) + jnp.roll(meridional, -1, axis=2)
    coupling = zonal_gain[None, :, None] * zonal_pair + meridional + 0.125 * corners
    return diagonal * centre - level_scale[:, None, None] * coupling


def operate(field, diagonal, level_scale, zonal_gain):
    midway = field.shape[2] // 2
    northern = jnp.roll(field[:, :1, :], midway, axis=2)
    southern = jnp.roll(field[:, -1:, :], midway, axis=2)
    padded = jnp.concatenate([northern, field, southern], axis=1)
    return stencil(padded, diagonal, level_scale, zonal_gain)


def reference(right_side, diag_shift, level_scale):
    levels, latitudes, longitudes = right_side.shape
    highest = lax.Precision.HIGHEST
    zonal_gain = polar_gain(latitudes, 0, latitudes)
    diagonal = diag_shift + level_scale[:, None, None] * (2.0 * zonal_gain[None, :, None] + 2.5)
    columns = jnp.arange(2 * WAVES, dtype=jnp.int32)
    wavenumber = columns % WAVES
    fourier = fourier_table(longitudes, wavenumber, columns < WAVES)
    sines = sine_table(latitudes)
    spectral = spectral_weights(latitudes, longitudes, wavenumber)

    def apply_inverse(current):
        coefficients = jnp.einsum("kjx,xc->kjc", current, fourier, precision=highest)
        modes = jnp.einsum("kjc,jl->klc", coefficients, sines, precision=highest) * spectral[None]
        returned = jnp.einsum("klc,jl->kjc", modes, sines, precision=highest)
        synthesis = jnp.einsum("kjc,xc->kjx", returned, fourier, precision=highest)
        return 0.5 * current / diagonal + synthesis

    solution = jnp.zeros_like(right_side)
    residual = right_side
    adjusted = apply_inverse(residual)
    aligned = jnp.sum(residual * adjusted)
    direction = adjusted
    for iteration in range(ITERS):
        image = operate(direction, diagonal, level_scale, zonal_gain)
        step_size = aligned / jnp.sum(direction * image)
        solution = solution + step_size * direction
        residual = residual - step_size * image
        if iteration + 1 < ITERS:
            adjusted = apply_inverse(residual)
            aligned_next = jnp.sum(residual * adjusted)
            direction = adjusted + (aligned_next / aligned) * direction
            aligned = aligned_next
    return solution, residual
```

```python
import functools

import jax
import jax.numpy as jnp
import numpy as np
from jax import lax
from jax.experimental import pallas as pl
from jax.experimental.pallas import tpu as pltpu
from jax.sharding import PartitionSpec as P

WAVES = 640
ITERS = 3
RADIX = 16
LANES = 128
SHIFT = 1.0
MESH = pl.DeviceIdType.MESH
F32 = jnp.float32


class Plan:
    def __init__(self, mesh, levels, rows, longitudes):
        self.bands, self.columns = mesh.shape["lat"], mesh.shape["lev"]
        self.levels, self.rows, self.longitudes = levels, rows, longitudes
        self.latitudes = rows * self.bands
        assert longitudes == RADIX * LANES and rows % 8 == 0
        self.groups = max(1, self.bands // RADIX)
        self.per = max(1, RADIX // self.bands)
        assert self.bands * self.per == RADIX * self.groups
        high = WAVES // RADIX
        self.quota = high // self.groups
        assert self.quota * self.groups == high and 2 * self.quota <= LANES
        self.halo = -(-self.per * levels * 2 // 8) * 8
        self.own = self.per * levels * rows
        self.chunk = self.own + self.halo

    def tables(self):
        n, lat = self.longitudes, self.latitudes
        m1, i2 = np.arange(RADIX), np.arange(LANES)
        angle = 2 * np.pi * ((m1[:, None] * i2[None]) % n) / n
        twiddle = np.stack([np.cos(angle), np.sin(angle)])
        twiddle = np.broadcast_to(twiddle[:, :, None, :], (2, RADIX, 8, LANES))
        zonal = np.zeros((2 * LANES, self.groups * LANES))
        waves = np.zeros((self.bands * self.per, 1, LANES))
        for g in range(self.groups):
            m2 = g * self.quota + np.arange(self.quota)
            phi = 2 * np.pi * ((i2[:, None] * m2[None]) % LANES) / LANES
            block = np.block([[np.cos(phi), np.sin(phi)], [-np.sin(phi), np.cos(phi)]])
            zonal[:, g * LANES : g * LANES + 2 * self.quota] = block
            for low in range(RADIX):
                part = 4 * np.sin(np.pi * (low + RADIX * m2) / n) ** 2
                waves[low * self.groups + g, 0, : 2 * self.quota] = np.tile(part, 2)
        count = np.arange(1, lat + 1)
        sines = np.sin(np.pi * ((count[:, None] * count[None]) % (2 * lat + 2)) / (lat + 1))
        edges = np.zeros((self.bands, 2, lat))
        edges[1:, 0] = sines[self.rows - 1 : lat - 1 : self.rows]
        edges[:-1, 1] = sines[self.rows :: self.rows]
        returned = np.concatenate([sines, edges.reshape(-1, lat)])
        merid = 4 * np.sin(0.5 * np.pi * count / (lat + 1)) ** 2
        merid = np.broadcast_to(merid[:, None], (lat, LANES))
        theta = np.pi * (4 * np.arange(lat) + 3) / (4 * lat + 2)
        gain = 1 / np.maximum(np.sin(theta), 0.5) ** 2
        gain = np.broadcast_to(gain.reshape(self.bands, self.rows, 1), (self.bands, self.rows, LANES))
        found = (twiddle, zonal, zonal.T, waves, sines, returned, merid, gain)
        return [jnp.asarray(np.ascontiguousarray(t), F32) for t in found]


def combine(terms):
    total = None
    for factor, value in terms:
        if abs(factor) < 1e-12:
            continue
        term = value if abs(factor - 1) < 1e-12 else (-value if abs(factor + 1) < 1e-12 else F32(factor) * value)
        total = term if total is None else total + term
    return total


COS = np.cos(2 * np.pi * np.arange(16) / 16)
SIN = np.sin(2 * np.pi * np.arange(16) / 16)


def fold(v):
    e = {i: v[i] + v[16 - i] for i in range(1, 8)}
    o = {i: v[i] - v[16 - i] for i in range(1, 8)}
    e[0], e[8] = v[0], v[8]
    even = {i: e[i] + e[8 - i] for i in range(4)}
    odd = {i: e[i] - e[8 - i] for i in range(4)}
    even[4] = e[4]
    same = {i: o[i] + o[8 - i] for i in range(1, 4)}
    diff = {i: o[i] - o[8 - i] for i in range(1, 4)}
    same[4] = o[4]
    p, q = {}, {}
    for k in range(9):
        source = even if k % 2 == 0 else odd
        p[k] = combine([(COS[i * k % 16], x) for i, x in source.items()])
        if 0 < k < 8:
            source = diff if k % 2 == 0 else same
            q[k] = combine([(SIN[i * k % 16], x) for i, x in source.items()])
    return p, q


def unfold(p, q):
    even = {i: combine([(COS[i * k % 16], p[k]) for k in range(0, 9, 2)]) for i in range(5)}
    odd = {i: combine([(COS[i * k % 16], p[k]) for k in range(1, 9, 2)]) for i in range(4)}
    same = {i: combine([(SIN[i * k % 16], q[k]) for k in range(1, 8, 2)]) for i in range(1, 5)}
    diff = {i: combine([(SIN[i * k % 16], q[k]) for k in range(2, 8, 2)]) for i in range(1, 4)}
    e, o = {4: even[4]}, {4: same[4]}
    for i in range(4):
        e[i], e[8 - i] = even[i] + odd[i], even[i] - odd[i]
    for i in range(1, 4):
        o[i], o[8 - i] = same[i] + diff[i], same[i] - diff[i]
    v = {0: e[0], 8: e[8]}
    for i in range(1, 8):
        v[i], v[16 - i] = e[i] + o[i], e[i] - o[i]
    return [v[i] for i in range(16)]


def dot(a, b):
    return jnp.dot(a, b, precision=lax.Precision.HIGHEST, preferred_element_type=F32)


def kernel(
    plan,
    scale_ref, side_ref, shift_ref, twiddle, zonal, zonal_t, waves, sines, returned, merid, gain_ref,
    x_ref, r_ref,
    diag, half, basis, image, edge, spectrum, filtered, moments,
    send_f, recv_f, send_b, recv_b, send_h, recv_h, part_a, recv_a, part_c, recv_c,
    sf, rf, sb, rb, sh, rh, sa, ra, sc, rc,
):
    bands, columns, levels, rows = plan.bands, plan.columns, plan.levels, plan.rows
    per, groups, n = plan.per, plan.groups, plan.longitudes
    me, seat = lax.axis_index("lat"), lax.axis_index("lev")
    pending = []

    barrier = pltpu.get_barrier_semaphore()
    for off in range(1, bands):
        pl.semaphore_signal(
            barrier, inc=1, device_id={"lat": lax.rem(me + off, bands)}, device_id_type=MESH
        )
    for off in range(1, columns):
        pl.semaphore_signal(
            barrier, inc=1, device_id={"lev": lax.rem(seat + off, columns)}, device_id_type=MESH
        )

    def push(src, dst, send_sem, recv_sem, target):
        copy = pltpu.make_async_remote_copy(
            src_ref=src, dst_ref=dst, send_sem=send_sem, recv_sem=recv_sem,
            device_id=target, device_id_type=MESH,
        )
        copy.start()
        pending.append(copy)
        return copy

    gain = jnp.concatenate([gain_ref[me]] * RADIX, axis=1)
    scales = [scale_ref[k] for k in range(levels)]
    for k in range(levels):
        full = shift_ref[k] + scales[k] * (2.0 * gain + 2.5)
        diag[k] = full
        half[k] = 0.5 / full

    def analyse(source, it):
        for k in range(levels):
            whole = source[k]
            scaled = half[k] * whole
            send_h[it, 0, k] = scaled[:1]
            send_h[it, 1, k] = scaled[rows - 1 :]
            for row in range(0, rows, 8):
                p, q = fold([whole[row : row + 8, LANES * i : LANES * (i + 1)] for i in range(RADIX)])
                for low in range(RADIX):
                    c, s = twiddle[0, low], twiddle[1, low]
                    fp = p[min(low, RADIX - low)]
                    if low % 8 == 0:
                        zc, zs = fp * c, fp * s
                    else:
                        fq = q[low] if low < 8 else -q[RADIX - low]
                        zc, zs = fp * c - fq * s, fp * s + fq * c
                    start = (low * levels + k) * rows + row
                    spectrum[start : start + 8, :LANES] = zc
                    spectrum[start : start + 8, LANES:] = zs
        found = dot(spectrum[...], zonal[...])
        for low in range(RADIX):
            for g in range(groups):
                block = found[low * levels * rows : (low + 1) * levels * rows, g * LANES : (g + 1) * LANES]
                send_f[it, low * groups + g] = block

    def exchange(it):
        mine = pl.ds(me * per, per)
        copies = []
        for off in range(1, bands):
            target = lax.rem(me + off, bands)
            copies.append(push(
                send_f.at[it, pl.ds(target * per, per)], recv_f.at[it, mine],
                sf.at[it, off], rf.at[it, off], {"lat": target},
            ))
        edges = [
            push(send_h.at[it, 0], recv_h.at[it, 1], sh.at[it, 0], rh.at[it, 0],
                 {"lat": lax.rem(me + bands - 1, bands)}),
            push(send_h.at[it, 1], recv_h.at[it, 0], sh.at[it, 1], rh.at[it, 1],
                 {"lat": lax.rem(me + 1, bands)}),
        ]
        recv_f[it, mine] = send_f[it, mine]
        return copies, edges

    def meridional(it):
        blocks = []
        for p in range(per):
            for k in range(levels):
                blocks.append(jnp.concatenate(
                    [recv_f[it, s * per + p, k * rows : (k + 1) * rows, :] for s in range(bands)], axis=0
                ))
        modes = dot(sines[...], jnp.concatenate(blocks, axis=1)) * filtered[...]
        back = dot(returned[...], modes)
        lat = plan.latitudes
        for b in range(bands):
            for i in range(per * levels):
                lanes = slice(i * LANES, (i + 1) * LANES)
                send_b[it, b, i * rows : (i + 1) * rows, :] = back[b * rows : (b + 1) * rows, lanes]
                start = plan.own + 2 * i
                send_b[it, b, start : start + 2, :] = back[lat + 2 * b : lat + 2 * b + 2, lanes]
        copies = []
        for off in range(1, bands):
            target = lax.rem(me + off, bands)
            copies.append(push(
                send_b.at[it, target], recv_b.at[it, me], sb.at[it, off], rb.at[it, off], {"lat": target},
            ))
        recv_b[it, me] = send_b[it, me]
        return copies

    def synthesise(it, source):
        left = []
        for low in range(RADIX):
            blocks = []
            for g in range(groups):
                unit = low * groups + g
                start = unit % per * levels * rows
                blocks.append(recv_b[it, unit // per, start : start + levels * rows, :])
            left.append(jnp.concatenate(blocks, axis=1))
        for h in range(RADIX // per):
            left.append(jnp.concatenate(
                [recv_b[it, h * groups + g, plan.own :, :] for g in range(groups)], axis=1
            ))
        found = dot(jnp.concatenate(left, axis=0), zonal_t[...])
        base = RADIX * levels * rows

        def gather(block_of):
            p, q = {}, {}
            for low in range(RADIX):
                block = block_of(low)
                c, s = twiddle[0, low], twiddle[1, low]
                real, imag = block[:, :LANES], block[:, LANES:]
                index = min(low, RADIX - low)
                fp = real * c + imag * s
                p[index] = fp if index not in p else p[index] + fp
                if low % 8:
                    fq = imag * c - real * s
                    q[index] = fq if low < 8 else q[index] - fq
            return jnp.concatenate(unfold(p, q), axis=1)

        def beside(low):
            h, p = low // per, low % per
            block = found[base + h * plan.halo : base + h * plan.halo + plan.halo]
            block = block[p * 2 * levels : (p + 1) * 2 * levels]
            fill = 8 - 2 * levels
            return block if fill == 0 else jnp.concatenate([block, jnp.zeros((fill, 2 * LANES), F32)], axis=0)

        for k in range(levels):
            for row in range(0, rows, 8):
                field = gather(
                    lambda low: found[(low * levels + k) * rows + row : (low * levels + k) * rows + row + 8]
                )
                piece = slice(row, row + 8)
                field = field + half[k, piece] * source[k, piece]
                if it > 0:
                    field = field - SHIFT * basis[it - 1, k, piece]
                basis[it, k, piece] = field
        edge[it] = gather(beside)

    def apply(it):
        middle = n // 2
        for k in range(levels):
            field = basis[it, k]
            outer = []
            for side in range(2):
                r = 2 * k + side
                line = edge[it, r : r + 1] + recv_h[it, side, k]
                if it > 0:
                    line = line - SHIFT * edge[it - 1, r : r + 1]
                own = field[:1] if side == 0 else field[rows - 1 :]
                pole = jnp.concatenate([own[:, middle:], own[:, :middle]], axis=1)
                line = jnp.where(me == (0 if side == 0 else bands - 1), pole, line)
                edge[it, r : r + 1] = line
                outer.append(line)
            number = lax.broadcasted_iota(jnp.int32, (rows, n), 0)
            north = jnp.where(number == 0, outer[0], pltpu.roll(field, 1, 0))
            south = jnp.where(number == rows - 1, outer[1], pltpu.roll(field, rows - 1, 0))
            pair = north + south
            mixed = gain * field + 0.125 * pair
            coupling = pltpu.roll(mixed, 1, 1) + pltpu.roll(mixed, n - 1, 1) + pair
            image[it, k] = diag[k] * field - scales[k] * coupling

    def product(a, b):
        total = None
        for k in range(levels):
            value = a[k] * b[k]
            for i in range(RADIX):
                for row in range(0, rows, 8):
                    term = value[row : row + 8, LANES * i : LANES * (i + 1)]
                    total = term if total is None else total + term
        return jnp.sum(total, axis=0, keepdims=True)

    def moment(index):
        for i in range(index + 1):
            moments[index * (ITERS + 1) + i] = product(basis.at[i], image.at[index])
        moments[index * (ITERS + 1) + ITERS] = product(basis.at[index], side_ref)

    source = side_ref
    for it in range(ITERS):
        analyse(source, it)
        if it == 0:
            pl.semaphore_wait(barrier, bands - 1 + columns - 1)
        copies, edges = exchange(it)
        if it == 0:
            scaling = 2.0 / (n * (plan.latitudes + 1))
            for p in range(per):
                weight = scaling / (1.0 + merid[...] + waves[me * per + p])
                for k in range(levels):
                    place = p * levels + k
                    filtered[:, place * LANES : (place + 1) * LANES] = weight
        else:
            moment(it - 1)
        for copy in copies:
            copy.wait_recv()
        copies = meridional(it)
        for copy in copies + edges:
            copy.wait_recv()
        synthesise(it, source)
        apply(it)
        source = image.at[it]
    moment(ITERS - 1)

    lane = lax.broadcasted_iota(jnp.int32, (1, LANES), 1)
    places = [(i, j) for j in range(ITERS) for i in list(range(j + 1)) + [ITERS]]
    row = jnp.zeros((1, LANES), F32)
    for at, (i, j) in enumerate(places):
        value = jnp.sum(moments[j * (ITERS + 1) + i], axis=1, keepdims=True)
        row = row + jnp.where(lane == at, value, 0.0)

    def gather_sum(part, received, value, axis, here, count, send_sems, recv_sems):
        part[...] = value
        copies = []
        for off in range(1, count):
            copies.append(push(
                part, received.at[here], send_sems.at[off], recv_sems.at[off],
                {axis: lax.rem(here + off, count)},
            ))
        received[here] = value
        for copy in copies:
            copy.wait_recv()
        total = received[0]
        for i in range(1, count):
            total = total + received[i]
        return total

    row = gather_sum(part_a, recv_a, row, "lat", me, bands, sa, ra)
    row = gather_sum(part_c, recv_c, row, "lev", seat, columns, sc, rc)
    gram, load = {}, {}
    for at, (i, j) in enumerate(places):
        value = jnp.sum(jnp.where(lane == at, row, 0.0), axis=1, keepdims=True)
        if i == ITERS:
            load[j] = value
        else:
            gram[j, i] = value
    pivot, lower = {}, {}
    for j in range(ITERS):
        for i in range(j):
            for m in range(i):
                gram[j, i] = gram[j, i] - gram[j, m] * lower[i, m]
            lower[j, i] = gram[j, i] / pivot[i]
        pivot[j] = gram[j, j]
        for i in range(j):
            pivot[j] = pivot[j] - lower[j, i] * gram[j, i]
            load[j] = load[j] - lower[j, i] * load[i]
    weight = {}
    for j in reversed(range(ITERS)):
        weight[j] = load[j] / pivot[j]
        for i in range(j + 1, ITERS):
            weight[j] = weight[j] - lower[i, j] * weight[i]
    for k in range(levels):
        total, left = None, side_ref[k]
        for i in range(ITERS):
            term = weight[i] * basis[i, k]
            total = term if total is None else total + term
            left = left - weight[i] * image[i, k]
        x_ref[k] = total
        r_ref[k] = left
    for copy in pending:
        copy.wait_send()


def body(mesh, right_side, diag_shift, level_scale):
    levels, rows, n = right_side.shape
    plan = Plan(mesh, levels, rows, n)
    bands, columns, per = plan.bands, plan.columns, plan.per
    field = jax.ShapeDtypeStruct(right_side.shape, F32)
    vmem = pl.BlockSpec(memory_space=pltpu.VMEM)
    dma = pltpu.SemaphoreType.DMA
    units, block = bands * per, levels * rows
    tables = plan.tables()
    return pl.pallas_call(
        functools.partial(kernel, plan),
        out_shape=(field, field),
        in_specs=[pl.BlockSpec(memory_space=pltpu.SMEM)] + [vmem] * (2 + len(tables)),
        out_specs=(vmem, vmem),
        scratch_shapes=[
            pltpu.VMEM((levels, rows, n), F32),
            pltpu.VMEM((levels, rows, n), F32),
            pltpu.VMEM((ITERS, levels, rows, n), F32),
            pltpu.VMEM((ITERS, levels, rows, n), F32),
            pltpu.VMEM((ITERS, 8, n), F32),
            pltpu.VMEM((RADIX * block, 2 * LANES), F32),
            pltpu.VMEM((plan.latitudes, per * levels * LANES), F32),
            pltpu.VMEM((ITERS * (ITERS + 1), 1, LANES), F32),
            pltpu.VMEM((ITERS, units, block, LANES), F32),
            pltpu.VMEM((ITERS, units, block, LANES), F32),
            pltpu.VMEM((ITERS, bands, plan.chunk, LANES), F32),
            pltpu.VMEM((ITERS, bands, plan.chunk, LANES), F32),
            pltpu.VMEM((ITERS, 2, levels, 1, n), F32),
            pltpu.VMEM((ITERS, 2, levels, 1, n), F32),
            pltpu.VMEM((1, LANES), F32),
            pltpu.VMEM((bands, 1, LANES), F32),
            pltpu.VMEM((1, LANES), F32),
            pltpu.VMEM((columns, 1, LANES), F32),
            dma((ITERS, bands)), dma((ITERS, bands)), dma((ITERS, bands)), dma((ITERS, bands)),
            dma((ITERS, 2)), dma((ITERS, 2)),
            dma((bands,)), dma((bands,)), dma((columns,)), dma((columns,)),
        ],
        compiler_params=pltpu.CompilerParams(collective_id=0, has_side_effects=True),
    )(level_scale, right_side, diag_shift, *tables)


def solution(mesh):
    placed = (P("lev", "lat", None), P("lev", "lat", None), P("lev"))
    return jax.shard_map(
        functools.partial(body, mesh),
        mesh=mesh,
        in_specs=placed,
        out_specs=(P("lev", "lat", None), P("lev", "lat", None)),
        check_vma=False,
    )
```

```python
import functools

import jax
import jax.numpy as jnp
import numpy as np
from jax import lax
from jax.experimental import pallas as pl
from jax.experimental.pallas import tpu as pltpu
from jax.sharding import PartitionSpec as P

WAVES = 640
ITERS = 3
RADIX = 16
LANES = 128
SHIFT = 1.0
MESH = pl.DeviceIdType.MESH
F32 = jnp.float32


class Plan:
    def __init__(self, mesh, levels, rows, longitudes):
        self.bands, self.columns = mesh.shape["lat"], mesh.shape["lev"]
        self.levels, self.rows, self.longitudes = levels, rows, longitudes
        self.latitudes = rows * self.bands
        assert longitudes == RADIX * LANES and rows % 8 == 0
        self.groups = max(1, self.bands // RADIX)
        self.per = max(1, RADIX // self.bands)
        assert self.bands * self.per == RADIX * self.groups
        high = WAVES // RADIX
        self.quota = high // self.groups
        assert self.quota * self.groups == high and 2 * self.quota <= LANES
        self.blocks = RADIX // self.per
        self.span = 2 * self.per * self.quota
        self.width = -(-self.span // LANES) * LANES
        self.tiles = max(-(-levels * self.span // LANES), self.width // LANES)
        self.lanes = self.tiles * LANES
        assert levels <= 4
        self.own = self.tiles * rows
        self.chunk = self.own + -(-2 * self.tiles // 8) * 8

    def tables(self):
        n, lat = self.longitudes, self.latitudes
        m1, i2 = np.arange(RADIX), np.arange(LANES)
        angle = 2 * np.pi * ((m1[:, None] * i2[None]) % n) / n
        twiddle = np.stack([np.cos(angle), np.sin(angle)])
        twiddle = np.broadcast_to(twiddle[:, :, None, :], (2, RADIX, 8, LANES))
        zonal = np.zeros((self.per * 2 * LANES, self.groups * self.width))
        waves = np.zeros((self.bands, 1, self.lanes))
        for g in range(self.groups):
            m2 = g * self.quota + np.arange(self.quota)
            phi = 2 * np.pi * ((i2[:, None] * m2[None]) % LANES) / LANES
            block = np.block([[np.cos(phi), np.sin(phi)], [-np.sin(phi), np.cos(phi)]])
            for p in range(self.per):
                start = g * self.width + 2 * p * self.quota
                zonal[2 * LANES * p : 2 * LANES * (p + 1), start : start + 2 * self.quota] = block
                for h in range(self.blocks):
                    part = 4 * np.sin(np.pi * (h * self.per + p + RADIX * m2) / n) ** 2
                    for k in range(self.levels):
                        start = k * self.span + 2 * p * self.quota
                        waves[h * self.groups + g, 0, start : start + 2 * self.quota] = np.tile(part, 2)
        count = np.arange(1, lat + 1)
        sines = np.sin(np.pi * ((count[:, None] * count[None]) % (2 * lat + 2)) / (lat + 1))
        edges = np.zeros((self.bands, 2, lat))
        edges[1:, 0] = sines[self.rows - 1 : lat - 1 : self.rows]
        edges[:-1, 1] = sines[self.rows :: self.rows]
        returned = np.concatenate([sines, edges.reshape(-1, lat)])
        merid = 4 * np.sin(0.5 * np.pi * count / (lat + 1)) ** 2
        merid = np.broadcast_to(merid[:, None], (lat, self.lanes))
        theta = np.pi * (4 * np.arange(lat) + 3) / (4 * lat + 2)
        gain = 1 / np.maximum(np.sin(theta), 0.5) ** 2
        gain = np.broadcast_to(gain.reshape(self.bands, self.rows, 1), (self.bands, self.rows, LANES))
        found = (twiddle, zonal, zonal.T, waves, sines, returned, merid, gain)
        return [jnp.asarray(np.ascontiguousarray(t), F32) for t in found]


def combine(terms):
    total = None
    for factor, value in terms:
        if abs(factor) < 1e-12:
            continue
        term = value if abs(factor - 1) < 1e-12 else (-value if abs(factor + 1) < 1e-12 else F32(factor) * value)
        total = term if total is None else total + term
    return total


COS = np.cos(2 * np.pi * np.arange(16) / 16)
SIN = np.sin(2 * np.pi * np.arange(16) / 16)


def fold(v):
    e = {i: v[i] + v[16 - i] for i in range(1, 8)}
    o = {i: v[i] - v[16 - i] for i in range(1, 8)}
    e[0], e[8] = v[0], v[8]
    even = {i: e[i] + e[8 - i] for i in range(4)}
    odd = {i: e[i] - e[8 - i] for i in range(4)}
    even[4] = e[4]
    same = {i: o[i] + o[8 - i] for i in range(1, 4)}
    diff = {i: o[i] - o[8 - i] for i in range(1, 4)}
    same[4] = o[4]
    p, q = {}, {}
    for k in range(9):
        source = even if k % 2 == 0 else odd
        p[k] = combine([(COS[i * k % 16], x) for i, x in source.items()])
        if 0 < k < 8:
            source = diff if k % 2 == 0 else same
            q[k] = combine([(SIN[i * k % 16], x) for i, x in source.items()])
    return p, q


def unfold(p, q):
    even = {i: combine([(COS[i * k % 16], p[k]) for k in range(0, 9, 2)]) for i in range(5)}
    odd = {i: combine([(COS[i * k % 16], p[k]) for k in range(1, 9, 2)]) for i in range(4)}
    same = {i: combine([(SIN[i * k % 16], q[k]) for k in range(1, 8, 2)]) for i in range(1, 5)}
    diff = {i: combine([(SIN[i * k % 16], q[k]) for k in range(2, 8, 2)]) for i in range(1, 4)}
    e, o = {4: even[4]}, {4: same[4]}
    for i in range(4):
        e[i], e[8 - i] = even[i] + odd[i], even[i] - odd[i]
    for i in range(1, 4):
        o[i], o[8 - i] = same[i] + diff[i], same[i] - diff[i]
    v = {0: e[0], 8: e[8]}
    for i in range(1, 8):
        v[i], v[16 - i] = e[i] + o[i], e[i] - o[i]
    return [v[i] for i in range(16)]


def dot(a, b):
    return jnp.dot(a, b, precision=lax.Precision.HIGHEST, preferred_element_type=F32)


def kernel(
    plan,
    scale_ref, side_ref, shift_ref, twiddle, zonal, zonal_t, waves, sines, returned, merid, gain_ref,
    x_ref, r_ref,
    diag, half, basis, image, edge, spectrum, lines, filtered, moments,
    send_f, recv_f, send_b, recv_b, send_h, recv_h, part, parts,
    sf, rf, sb, rb, sh, rh, sa, ra,
):
    bands, columns, levels, rows = plan.bands, plan.columns, plan.levels, plan.rows
    per, groups, n = plan.per, plan.groups, plan.longitudes
    me, seat = lax.axis_index("lat"), lax.axis_index("lev")
    pending = []

    barrier = pltpu.get_barrier_semaphore()
    for i in range(bands):
        for j in range(columns):
            if (i, j) != (0, 0):
                pl.semaphore_signal(
                    barrier, inc=1, device_id_type=MESH,
                    device_id={"lat": lax.rem(me + i, bands), "lev": lax.rem(seat + j, columns)},
                )

    def push(src, dst, send_sem, recv_sem, target):
        copy = pltpu.make_async_remote_copy(
            src_ref=src, dst_ref=dst, send_sem=send_sem, recv_sem=recv_sem,
            device_id=target, device_id_type=MESH,
        )
        copy.start()
        pending.append(copy)
        return copy

    gain = jnp.concatenate([gain_ref[me]] * RADIX, axis=1)
    scales = [scale_ref[k] for k in range(levels)]
    for k in range(levels):
        full = shift_ref[k] + scales[k] * (2.0 * gain + 2.5)
        diag[k] = full
        half[k] = 0.5 / full

    def widen(block):
        if plan.width == plan.lanes:
            return block
        return jnp.concatenate([block, jnp.zeros((rows, plan.lanes - plan.width), F32)], axis=1)

    def turn(block, amount):
        amount = amount % plan.lanes
        return block if amount == 0 else pltpu.roll(block, amount, 1)

    def analyse(source, it):
        for k in range(levels):
            whole = source[k]
            scaled = half[k] * whole
            send_h[it, 0, k] = scaled[:1]
            send_h[it, 1, k] = scaled[rows - 1 :]
            for row in range(0, rows, 8):
                p, q = fold([whole[row : row + 8, LANES * i : LANES * (i + 1)] for i in range(RADIX)])
                for low in range(RADIX):
                    c, s = twiddle[0, low], twiddle[1, low]
                    fp = p[min(low, RADIX - low)]
                    if low % 8 == 0:
                        zc, zs = fp * c, fp * s
                    else:
                        fq = q[low] if low < 8 else -q[RADIX - low]
                        zc, zs = fp * c - fq * s, fp * s + fq * c
                    start = (low // per * levels + k) * rows + row
                    column = low % per * 2 * LANES
                    spectrum[start : start + 8, column : column + LANES] = zc
                    spectrum[start : start + 8, column + LANES : column + 2 * LANES] = zs
        found = dot(spectrum[...], zonal[...])
        for h in range(plan.blocks):
            for g in range(groups):
                total = None
                for k in range(levels):
                    start = (h * levels + k) * rows
                    block = found[start : start + rows, g * plan.width : (g + 1) * plan.width]
                    block = turn(widen(block), k * plan.span)
                    total = block if total is None else total + block
                send_f[it, h * groups + g] = total

    def spread(source, received, it, send_sems, recv_sems):
        copies = []
        for i in range(bands - 1):
            up = bands - 1 - i - (bands - 1 - i <= me).astype(jnp.int32)
            down = i + (i >= me).astype(jnp.int32)
            target = jnp.where(me < bands // 2, up, down)
            copies.append(push(
                source.at[it, target], received.at[it, me], send_sems.at[it, target], recv_sems.at[it, me],
                {"lat": target},
            ))
        received[it, me] = source[it, me]
        return [arrival(received, it, lax.rem(me + off, bands), recv_sems) for off in range(1, bands)]

    def arrival(received, it, sender, recv_sems):
        return pltpu.make_async_remote_copy(
            src_ref=received.at[it, sender], dst_ref=received.at[it, sender],
            send_sem=recv_sems.at[it, sender], recv_sem=recv_sems.at[it, sender],
            device_id={"lat": sender}, device_id_type=MESH,
        )

    def exchange(it):
        copies = spread(send_f, recv_f, it, sf, rf)
        edges = []
        for side, other in ((0, bands - 1), (1, 1)):
            copy = pltpu.make_async_remote_copy(
                src_ref=send_h.at[it, side], dst_ref=recv_h.at[it, 1 - side],
                send_sem=sh.at[it, side], recv_sem=rh.at[it, side],
                device_id={"lat": lax.rem(me + other, bands)}, device_id_type=MESH,
            )
            edges.append(copy)
            pl.when(me != (bands - 1) * side)(copy.start)
        return copies, edges

    def meridional(it):
        received = jnp.concatenate([recv_f[it, s] for s in range(bands)], axis=0)
        modes = dot(sines[...], received) * filtered[...]
        back = dot(returned[...], modes)
        lat = plan.latitudes
        for b in range(bands):
            for t in range(plan.tiles):
                lanes = slice(t * LANES, (t + 1) * LANES)
                send_b[it, b, t * rows : (t + 1) * rows, :] = back[b * rows : (b + 1) * rows, lanes]
                start = plan.own + 2 * t
                send_b[it, b, start : start + 2, :] = back[lat + 2 * b : lat + 2 * b + 2, lanes]
        return spread(send_b, recv_b, it, sb, rb)

    def synthesise(it, source):
        left = []
        for h in range(plan.blocks):
            for k in range(levels):
                wide = []
                for g in range(groups):
                    parts = [recv_b[it, h * groups + g, t * rows : (t + 1) * rows, :] for t in range(plan.tiles)]
                    wide.append(turn(jnp.concatenate(parts, axis=1), -k * plan.span)[:, : plan.width])
                left.append(jnp.concatenate(wide, axis=1))
        for h in range(plan.blocks):
            for g in range(groups):
                for t in range(plan.tiles):
                    start = g * plan.lanes + t * LANES
                    pair = recv_b[it, h * groups + g, plan.own + 2 * t : plan.own + 2 * t + 2, :]
                    for k in range(levels):
                        lines[h, 2 * k : 2 * k + 2, start : start + LANES] = pair
            level = lax.broadcasted_iota(jnp.int32, (8, plan.lanes), 0) // 2
            wide = []
            for g in range(groups):
                both = lines[h, :, g * plan.lanes : (g + 1) * plan.lanes]
                found = both
                for k in range(1, levels):
                    found = jnp.where(level == k, turn(both, -k * plan.span), found)
                wide.append(found[:, : plan.width])
            left.append(jnp.concatenate(wide, axis=1))
        found = dot(jnp.concatenate(left, axis=0), zonal_t[...])
        base = plan.blocks * levels * rows

        def gather(block_of):
            p, q = {}, {}
            for low in range(RADIX):
                block = block_of(low)
                c, s = twiddle[0, low], twiddle[1, low]
                real, imag = block[:, :LANES], block[:, LANES:]
                index = min(low, RADIX - low)
                fp = real * c + imag * s
                p[index] = fp if index not in p else p[index] + fp
                if low % 8:
                    fq = imag * c - real * s
                    q[index] = fq if low < 8 else q[index] - fq
            return jnp.concatenate(unfold(p, q), axis=1)

        def cut(start, low):
            column = low % per * 2 * LANES
            return found[start : start + 8, column : column + 2 * LANES]

        def beside(low):
            return cut(base + low // per * 8, low)

        for k in range(levels):
            for row in range(0, rows, 8):
                field = gather(
                    lambda low: cut((low // per * levels + k) * rows + row, low)
                )
                piece = slice(row, row + 8)
                field = field + half[k, piece] * source[k, piece]
                if it > 0:
                    field = field - SHIFT * basis[it - 1, k, piece]
                basis[it, k, piece] = field
        edge[it] = gather(beside)

    def apply(it):
        middle = n // 2
        for k in range(levels):
            field = basis[it, k]
            outer = []
            for side in range(2):
                r = 2 * k + side
                line = edge[it, r : r + 1] + recv_h[it, side, k]
                if it > 0:
                    line = line - SHIFT * edge[it - 1, r : r + 1]
                own = field[:1] if side == 0 else field[rows - 1 :]
                pole = jnp.concatenate([own[:, middle:], own[:, :middle]], axis=1)
                line = jnp.where(me == (0 if side == 0 else bands - 1), pole, line)
                edge[it, r : r + 1] = line
                outer.append(line)
            number = lax.broadcasted_iota(jnp.int32, (rows, n), 0)
            north = jnp.where(number == 0, outer[0], pltpu.roll(field, 1, 0))
            south = jnp.where(number == rows - 1, outer[1], pltpu.roll(field, rows - 1, 0))
            pair = north + south
            mixed = gain * field + 0.125 * pair
            coupling = pltpu.roll(mixed, 1, 1) + pltpu.roll(mixed, n - 1, 1) + pair
            image[it, k] = diag[k] * field - scales[k] * coupling

    def product(a, b):
        total = None
        for k in range(levels):
            value = a[k] * b[k]
            for i in range(RADIX):
                for row in range(0, rows, 8):
                    term = value[row : row + 8, LANES * i : LANES * (i + 1)]
                    total = term if total is None else total + term
        return jnp.sum(total, axis=0, keepdims=True)

    def moment(index):
        for i in range(index + 1):
            moments[index * (ITERS + 1) + i] = product(basis.at[i], image.at[index])
        moments[index * (ITERS + 1) + ITERS] = product(basis.at[index], side_ref)

    source, beside = side_ref, []
    for it in range(ITERS):
        analyse(source, it)
        if it == 0:
            pl.semaphore_wait(barrier, bands * columns - 1)
        copies, edges = exchange(it)
        if it == 0:
            scaling = 2.0 / (n * (plan.latitudes + 1))
            filtered[...] = scaling / (1.0 + merid[...] + waves[me])
        else:
            moment(it - 1)
        for copy in copies:
            copy.wait_recv()
        copies = meridional(it)
        for copy in copies:
            copy.wait_recv()
        for side in range(2):
            pl.when(me != (bands - 1) * (1 - side))(edges[side].wait_recv)
            beside.append((side, edges[side]))
        synthesise(it, source)
        apply(it)
        source = image.at[it]
    moment(ITERS - 1)

    lane = lax.broadcasted_iota(jnp.int32, (1, LANES), 1)
    places = [(i, j) for j in range(ITERS) for i in list(range(j + 1)) + [ITERS]]
    row = jnp.zeros((1, LANES), F32)
    for at, (i, j) in enumerate(places):
        value = jnp.sum(moments[j * (ITERS + 1) + i], axis=1, keepdims=True)
        row = row + jnp.where(lane == at, value, 0.0)

    part[...] = row
    arrivals = []
    for i in range(bands - 1, -1, -1):
        for j in range(columns):
            if (i, j) != (0, 0):
                copy = push(
                    part, parts.at[me, seat], sa.at[i, j], ra.at[i, j],
                    {"lat": lax.rem(me + i, bands), "lev": lax.rem(seat + j, columns)},
                )
                arrivals.append(copy)
    parts[me, seat] = row
    for copy in arrivals:
        copy.wait_recv()
    row = jnp.sum(parts[...].reshape(bands * columns, LANES), axis=0, keepdims=True)
    gram, load = {}, {}
    for at, (i, j) in enumerate(places):
        value = jnp.sum(jnp.where(lane == at, row, 0.0), axis=1, keepdims=True)
        if i == ITERS:
            load[j] = value
        else:
            gram[j, i] = value
    pivot, lower = {}, {}
    for j in range(ITERS):
        for i in range(j):
            for m in range(i):
                gram[j, i] = gram[j, i] - gram[j, m] * lower[i, m]
            lower[j, i] = gram[j, i] / pivot[i]
        pivot[j] = gram[j, j]
        for i in range(j):
            pivot[j] = pivot[j] - lower[j, i] * gram[j, i]
            load[j] = load[j] - lower[j, i] * load[i]
    weight = {}
    for j in reversed(range(ITERS)):
        weight[j] = load[j] / pivot[j]
        for i in range(j + 1, ITERS):
            weight[j] = weight[j] - lower[i, j] * weight[i]
    for k in range(levels):
        total, left = None, side_ref[k]
        for i in range(ITERS):
            term = weight[i] * basis[i, k]
            total = term if total is None else total + term
            left = left - weight[i] * image[i, k]
        x_ref[k] = total
        r_ref[k] = left
    for copy in pending:
        copy.wait_send()
    for side, copy in beside:
        pl.when(me != (bands - 1) * side)(copy.wait_send)


def body(mesh, right_side, diag_shift, level_scale):
    levels, rows, n = right_side.shape
    plan = Plan(mesh, levels, rows, n)
    bands, columns, per = plan.bands, plan.columns, plan.per
    field = jax.ShapeDtypeStruct(right_side.shape, F32)
    vmem = pl.BlockSpec(memory_space=pltpu.VMEM)
    dma = pltpu.SemaphoreType.DMA
    block = levels * rows
    tables = plan.tables()
    return pl.pallas_call(
        functools.partial(kernel, plan),
        out_shape=(field, field),
        in_specs=[pl.BlockSpec(memory_space=pltpu.SMEM)] + [vmem] * (2 + len(tables)),
        out_specs=(vmem, vmem),
        scratch_shapes=[
            pltpu.VMEM((levels, rows, n), F32),
            pltpu.VMEM((levels, rows, n), F32),
            pltpu.VMEM((ITERS, levels, rows, n), F32),
            pltpu.VMEM((ITERS, levels, rows, n), F32),
            pltpu.VMEM((ITERS, 8, n), F32),
            pltpu.VMEM((plan.blocks * block, per * 2 * LANES), F32),
            pltpu.VMEM((plan.blocks, 8, plan.groups * plan.lanes), F32),
            pltpu.VMEM((plan.latitudes, plan.lanes), F32),
            pltpu.VMEM((ITERS * (ITERS + 1), 1, LANES), F32),
            pltpu.VMEM((ITERS, bands, rows, plan.lanes), F32),
            pltpu.VMEM((ITERS, bands, rows, plan.lanes), F32),
            pltpu.VMEM((ITERS, bands, plan.chunk, LANES), F32),
            pltpu.VMEM((ITERS, bands, plan.chunk, LANES), F32),
            pltpu.VMEM((ITERS, 2, levels, 1, n), F32),
            pltpu.VMEM((ITERS, 2, levels, 1, n), F32),
            pltpu.VMEM((1, LANES), F32),
            pltpu.VMEM((bands, columns, 1, LANES), F32),
            dma((ITERS, bands)), dma((ITERS, bands)), dma((ITERS, bands)), dma((ITERS, bands)),
            dma((ITERS, 2)), dma((ITERS, 2)),
            dma((bands, columns)), dma((bands, columns)),
        ],
        compiler_params=pltpu.CompilerParams(collective_id=0, has_side_effects=True),
    )(level_scale, right_side, diag_shift, *tables)


def solution(mesh):
    placed = (P("lev", "lat", None), P("lev", "lat", None), P("lev"))
    return jax.shard_map(
        functools.partial(body, mesh),
        mesh=mesh,
        in_specs=placed,
        out_specs=(P("lev", "lat", None), P("lev", "lat", None)),
        check_vma=False,
    )
```

```python
import functools

import jax
import jax.numpy as jnp
import numpy as np
from jax import lax
from jax.experimental import pallas as pl
from jax.experimental.pallas import tpu as pltpu
from jax.sharding import PartitionSpec as P

WAVES = 640
ITERS = 3
RADIX = 16
LANES = 128
SHIFT = 1.0
MESH = pl.DeviceIdType.MESH
F32 = jnp.float32


class Plan:
    def __init__(self, mesh, levels, rows, longitudes):
        self.bands, self.columns = mesh.shape["lat"], mesh.shape["lev"]
        self.levels, self.rows, self.longitudes = levels, rows, longitudes
        self.latitudes = rows * self.bands
        assert longitudes == RADIX * LANES and rows % 8 == 0
        self.groups = max(1, self.bands // RADIX)
        self.per = max(1, RADIX // self.bands)
        assert self.bands * self.per == RADIX * self.groups
        high = WAVES // RADIX
        self.quota = high // self.groups
        assert self.quota * self.groups == high and 2 * self.quota <= LANES
        self.blocks = RADIX // self.per
        self.span = 2 * self.per * self.quota
        self.width = -(-self.span // LANES) * LANES
        self.tiles = max(-(-levels * self.span // LANES), self.width // LANES)
        self.lanes = self.tiles * LANES
        assert levels <= 4
        self.own = self.tiles * rows
        self.chunk = self.own + -(-2 * self.tiles // 8) * 8

    def tables(self):
        n, lat = self.longitudes, self.latitudes
        m1, i2 = np.arange(RADIX), np.arange(LANES)
        angle = 2 * np.pi * ((m1[:, None] * i2[None]) % n) / n
        twiddle = np.stack([np.cos(angle), np.sin(angle)])
        twiddle = np.broadcast_to(twiddle[:, :, None, :], (2, RADIX, 8, LANES))
        zonal = np.zeros((self.per * 2 * LANES, self.groups * self.width))
        waves = np.zeros((self.bands, 1, self.lanes))
        for g in range(self.groups):
            m2 = g * self.quota + np.arange(self.quota)
            phi = 2 * np.pi * ((i2[:, None] * m2[None]) % LANES) / LANES
            block = np.block([[np.cos(phi), np.sin(phi)], [-np.sin(phi), np.cos(phi)]])
            for p in range(self.per):
                start = g * self.width + 2 * p * self.quota
                zonal[2 * LANES * p : 2 * LANES * (p + 1), start : start + 2 * self.quota] = block
                for h in range(self.blocks):
                    part = 4 * np.sin(np.pi * (h * self.per + p + RADIX * m2) / n) ** 2
                    for k in range(self.levels):
                        start = k * self.span + 2 * p * self.quota
                        waves[h * self.groups + g, 0, start : start + 2 * self.quota] = np.tile(part, 2)
        count = np.arange(1, lat + 1)
        sines = np.sin(np.pi * ((count[:, None] * count[None]) % (2 * lat + 2)) / (lat + 1))
        edges = np.zeros((self.bands, 2, lat))
        edges[1:, 0] = sines[self.rows - 1 : lat - 1 : self.rows]
        edges[:-1, 1] = sines[self.rows :: self.rows]
        returned = np.concatenate([sines, edges.reshape(-1, lat)])
        merid = 4 * np.sin(0.5 * np.pi * count / (lat + 1)) ** 2
        merid = np.broadcast_to(merid[:, None], (lat, self.lanes))
        theta = np.pi * (4 * np.arange(lat) + 3) / (4 * lat + 2)
        gain = 1 / np.maximum(np.sin(theta), 0.5) ** 2
        gain = np.broadcast_to(gain.reshape(self.bands, self.rows, 1), (self.bands, self.rows, LANES))
        found = (twiddle, zonal, zonal.T, waves, sines, returned, merid, gain)
        return [jnp.asarray(np.ascontiguousarray(t), F32) for t in found]


def combine(terms):
    total = None
    for factor, value in terms:
        if abs(factor) < 1e-12:
            continue
        term = value if abs(factor - 1) < 1e-12 else (-value if abs(factor + 1) < 1e-12 else F32(factor) * value)
        total = term if total is None else total + term
    return total


COS = np.cos(2 * np.pi * np.arange(16) / 16)
SIN = np.sin(2 * np.pi * np.arange(16) / 16)


def fold(v):
    e = {i: v[i] + v[16 - i] for i in range(1, 8)}
    o = {i: v[i] - v[16 - i] for i in range(1, 8)}
    e[0], e[8] = v[0], v[8]
    even = {i: e[i] + e[8 - i] for i in range(4)}
    odd = {i: e[i] - e[8 - i] for i in range(4)}
    even[4] = e[4]
    same = {i: o[i] + o[8 - i] for i in range(1, 4)}
    diff = {i: o[i] - o[8 - i] for i in range(1, 4)}
    same[4] = o[4]
    p, q = {}, {}
    for k in range(9):
        source = even if k % 2 == 0 else odd
        p[k] = combine([(COS[i * k % 16], x) for i, x in source.items()])
        if 0 < k < 8:
            source = diff if k % 2 == 0 else same
            q[k] = combine([(SIN[i * k % 16], x) for i, x in source.items()])
    return p, q


def unfold(p, q):
    even = {i: combine([(COS[i * k % 16], p[k]) for k in range(0, 9, 2)]) for i in range(5)}
    odd = {i: combine([(COS[i * k % 16], p[k]) for k in range(1, 9, 2)]) for i in range(4)}
    same = {i: combine([(SIN[i * k % 16], q[k]) for k in range(1, 8, 2)]) for i in range(1, 5)}
    diff = {i: combine([(SIN[i * k % 16], q[k]) for k in range(2, 8, 2)]) for i in range(1, 4)}
    e, o = {4: even[4]}, {4: same[4]}
    for i in range(4):
        e[i], e[8 - i] = even[i] + odd[i], even[i] - odd[i]
    for i in range(1, 4):
        o[i], o[8 - i] = same[i] + diff[i], same[i] - diff[i]
    v = {0: e[0], 8: e[8]}
    for i in range(1, 8):
        v[i], v[16 - i] = e[i] + o[i], e[i] - o[i]
    return [v[i] for i in range(16)]


def dot(a, b):
    return jnp.dot(a, b, precision=lax.Precision.HIGHEST, preferred_element_type=F32)


def kernel(
    plan,
    scale_ref, side_ref, shift_ref, twiddle, zonal, zonal_t, waves, sines, returned, merid, gain_ref,
    out_ref,
    diag, half, basis, image, edge, spectrum, lines, filtered, moments,
    send_f, recv_f, send_b, recv_b, send_h, recv_h, part, parts,
    sf, rf, sb, rb, sh, rh, sa, ra,
):
    bands, columns, levels, rows = plan.bands, plan.columns, plan.levels, plan.rows
    per, groups, n = plan.per, plan.groups, plan.longitudes
    me, seat = lax.axis_index("lat"), lax.axis_index("lev")
    pending = []

    barrier = pltpu.get_barrier_semaphore()
    for i in range(bands):
        for j in range(columns):
            if (i, j) != (0, 0):
                pl.semaphore_signal(
                    barrier, inc=1, device_id_type=MESH,
                    device_id={"lat": lax.rem(me + i, bands), "lev": lax.rem(seat + j, columns)},
                )

    def push(src, dst, send_sem, recv_sem, target):
        copy = pltpu.make_async_remote_copy(
            src_ref=src, dst_ref=dst, send_sem=send_sem, recv_sem=recv_sem,
            device_id=target, device_id_type=MESH,
        )
        copy.start()
        pending.append(copy)
        return copy

    gain = jnp.concatenate([gain_ref[me]] * RADIX, axis=1)
    scales = [scale_ref[k] for k in range(levels)]
    for k in range(levels):
        full = shift_ref[k] + scales[k] * (2.0 * gain + 2.5)
        diag[k] = full
        half[k] = 0.5 / full

    def widen(block):
        if plan.width == plan.lanes:
            return block
        return jnp.concatenate([block, jnp.zeros((rows, plan.lanes - plan.width), F32)], axis=1)

    def turn(block, amount):
        amount = amount % plan.lanes
        return block if amount == 0 else pltpu.roll(block, amount, 1)

    def analyse(source, it):
        for k in range(levels):
            whole = source[k]
            scaled = half[k] * whole
            send_h[it, 0, k] = scaled[:1]
            send_h[it, 1, k] = scaled[rows - 1 :]
            for row in range(0, rows, 8):
                p, q = fold([whole[row : row + 8, LANES * i : LANES * (i + 1)] for i in range(RADIX)])
                for low in range(RADIX):
                    c, s = twiddle[0, low], twiddle[1, low]
                    fp = p[min(low, RADIX - low)]
                    if low % 8 == 0:
                        zc, zs = fp * c, fp * s
                    else:
                        fq = q[low] if low < 8 else -q[RADIX - low]
                        zc, zs = fp * c - fq * s, fp * s + fq * c
                    start = (low // per * levels + k) * rows + row
                    column = low % per * 2 * LANES
                    spectrum[start : start + 8, column : column + LANES] = zc
                    spectrum[start : start + 8, column + LANES : column + 2 * LANES] = zs
        found = dot(spectrum[...], zonal[...])
        for h in range(plan.blocks):
            for g in range(groups):
                total = None
                for k in range(levels):
                    start = (h * levels + k) * rows
                    block = found[start : start + rows, g * plan.width : (g + 1) * plan.width]
                    block = turn(widen(block), k * plan.span)
                    total = block if total is None else total + block
                send_f[it, h * groups + g] = total

    def spread(source, received, it, send_sems, recv_sems):
        copies = []
        for i in range(bands - 1):
            up = bands - 1 - i - (bands - 1 - i <= me).astype(jnp.int32)
            down = i + (i >= me).astype(jnp.int32)
            target = jnp.where(me < bands // 2, up, down)
            copies.append(push(
                source.at[it, target], received.at[it, me], send_sems.at[it, target], recv_sems.at[it, me],
                {"lat": target},
            ))
        received[it, me] = source[it, me]
        return [arrival(received, it, lax.rem(me + off, bands), recv_sems) for off in range(1, bands)]

    def arrival(received, it, sender, recv_sems):
        return pltpu.make_async_remote_copy(
            src_ref=received.at[it, sender], dst_ref=received.at[it, sender],
            send_sem=recv_sems.at[it, sender], recv_sem=recv_sems.at[it, sender],
            device_id={"lat": sender}, device_id_type=MESH,
        )

    def exchange(it):
        copies = spread(send_f, recv_f, it, sf, rf)
        edges = []
        for side, other in ((0, bands - 1), (1, 1)):
            copy = pltpu.make_async_remote_copy(
                src_ref=send_h.at[it, side], dst_ref=recv_h.at[it, 1 - side],
                send_sem=sh.at[it, side], recv_sem=rh.at[it, side],
                device_id={"lat": lax.rem(me + other, bands)}, device_id_type=MESH,
            )
            edges.append(copy)
            pl.when(me != (bands - 1) * side)(copy.start)
        return copies, edges

    def meridional(it):
        received = jnp.concatenate([recv_f[it, s] for s in range(bands)], axis=0)
        modes = dot(sines[...], received) * filtered[...]
        back = dot(returned[...], modes)
        lat = plan.latitudes
        for b in range(bands):
            for t in range(plan.tiles):
                lanes = slice(t * LANES, (t + 1) * LANES)
                send_b[it, b, t * rows : (t + 1) * rows, :] = back[b * rows : (b + 1) * rows, lanes]
                start = plan.own + 2 * t
                send_b[it, b, start : start + 2, :] = back[lat + 2 * b : lat + 2 * b + 2, lanes]
        return spread(send_b, recv_b, it, sb, rb)

    def synthesise(it):
        left = []
        for h in range(plan.blocks):
            for k in range(levels):
                wide = []
                for g in range(groups):
                    parts = [recv_b[it, h * groups + g, t * rows : (t + 1) * rows, :] for t in range(plan.tiles)]
                    wide.append(turn(jnp.concatenate(parts, axis=1), -k * plan.span)[:, : plan.width])
                left.append(jnp.concatenate(wide, axis=1))
        for h in range(plan.blocks):
            for g in range(groups):
                for t in range(plan.tiles):
                    start = g * plan.lanes + t * LANES
                    pair = recv_b[it, h * groups + g, plan.own + 2 * t : plan.own + 2 * t + 2, :]
                    for k in range(levels):
                        lines[h, 2 * k : 2 * k + 2, start : start + LANES] = pair
            level = lax.broadcasted_iota(jnp.int32, (8, plan.lanes), 0) // 2
            wide = []
            for g in range(groups):
                both = lines[h, :, g * plan.lanes : (g + 1) * plan.lanes]
                found = both
                for k in range(1, levels):
                    found = jnp.where(level == k, turn(both, -k * plan.span), found)
                wide.append(found[:, : plan.width])
            left.append(jnp.concatenate(wide, axis=1))
        found = dot(jnp.concatenate(left, axis=0), zonal_t[...])
        base = plan.blocks * levels * rows

        def gather(block_of):
            p, q = {}, {}
            for low in range(RADIX):
                block = block_of(low)
                c, s = twiddle[0, low], twiddle[1, low]
                real, imag = block[:, :LANES], block[:, LANES:]
                index = min(low, RADIX - low)
                fp = real * c + imag * s
                p[index] = fp if index not in p else p[index] + fp
                if low % 8:
                    fq = imag * c - real * s
                    q[index] = fq if low < 8 else q[index] - fq
            return jnp.concatenate(unfold(p, q), axis=1)

        def cut(start, low):
            column = low % per * 2 * LANES
            return found[start : start + 8, column : column + 2 * LANES]

        def beside(low):
            return cut(base + low // per * 8, low)

        for k in range(levels):
            for row in range(0, rows, 8):
                field = gather(
                    lambda low: cut((low // per * levels + k) * rows + row, low)
                )
                piece = slice(row, row + 8)
                basis[it, k, piece] = field + basis[it, k, piece]
        edge[it] = gather(beside)

    def apply(it):
        middle = n // 2
        for k in range(levels):
            field = basis[it, k]
            outer = []
            for side in range(2):
                r = 2 * k + side
                line = edge[it, r : r + 1] + recv_h[it, side, k]
                if it > 0:
                    line = line - SHIFT * edge[it - 1, r : r + 1]
                own = field[:1] if side == 0 else field[rows - 1 :]
                pole = jnp.concatenate([own[:, middle:], own[:, :middle]], axis=1)
                line = jnp.where(me == (0 if side == 0 else bands - 1), pole, line)
                edge[it, r : r + 1] = line
                outer.append(line)
            number = lax.broadcasted_iota(jnp.int32, (rows, n), 0)
            north = jnp.where(number == 0, outer[0], pltpu.roll(field, 1, 0))
            south = jnp.where(number == rows - 1, outer[1], pltpu.roll(field, rows - 1, 0))
            pair = north + south
            mixed = gain * field + 0.125 * pair
            coupling = pltpu.roll(mixed, 1, 1) + pltpu.roll(mixed, n - 1, 1) + pair
            image[it, k] = diag[k] * field - scales[k] * coupling

    def product(a, b):
        total = None
        for k in range(levels):
            value = a[k] * b[k]
            for i in range(RADIX):
                for row in range(0, rows, 8):
                    term = value[row : row + 8, LANES * i : LANES * (i + 1)]
                    total = term if total is None else total + term
        return jnp.sum(total, axis=0, keepdims=True)

    def moment(index):
        for i in range(index + 1):
            moments[index * (ITERS + 1) + i] = product(basis.at[i], image.at[index])
        moments[index * (ITERS + 1) + ITERS] = product(basis.at[index], side_ref)

    source, beside = side_ref, []
    for it in range(ITERS):
        analyse(source, it)
        if it == 0:
            pl.semaphore_wait(barrier, bands * columns - 1)
        copies, edges = exchange(it)
        if it == 0:
            scaling = 2.0 / (n * (plan.latitudes + 1))
            filtered[...] = scaling / (1.0 + merid[...] + waves[me])
        else:
            moment(it - 1)
        for copy in copies:
            copy.wait_recv()
        copies = meridional(it)
        for k in range(levels):
            known = half[k] * source[k]
            basis[it, k] = known - SHIFT * basis[it - 1, k] if it > 0 else known
        for copy in copies:
            copy.wait_recv()
        for side in range(2):
            pl.when(me != (bands - 1) * (1 - side))(edges[side].wait_recv)
            beside.append((side, edges[side]))
        synthesise(it)
        apply(it)
        source = image.at[it]
    moment(ITERS - 1)

    lane = lax.broadcasted_iota(jnp.int32, (1, LANES), 1)
    places = [(i, j) for j in range(ITERS) for i in list(range(j + 1)) + [ITERS]]
    row = jnp.zeros((1, LANES), F32)
    for at, (i, j) in enumerate(places):
        value = jnp.sum(moments[j * (ITERS + 1) + i], axis=1, keepdims=True)
        row = row + jnp.where(lane == at, value, 0.0)

    part[...] = row
    arrivals = []
    for i in range(bands - 1, -1, -1):
        for j in range(columns):
            if (i, j) != (0, 0):
                copy = push(
                    part, parts.at[me, seat], sa.at[i, j], ra.at[i, j],
                    {"lat": lax.rem(me + i, bands), "lev": lax.rem(seat + j, columns)},
                )
                arrivals.append(copy)
    parts[me, seat] = row
    for copy in arrivals:
        copy.wait_recv()
    row = jnp.sum(parts[...].reshape(bands * columns, LANES), axis=0, keepdims=True)
    gram, load = {}, {}
    for at, (i, j) in enumerate(places):
        value = jnp.sum(jnp.where(lane == at, row, 0.0), axis=1, keepdims=True)
        if i == ITERS:
            load[j] = value
        else:
            gram[j, i] = value
    pivot, lower = {}, {}
    for j in range(ITERS):
        for i in range(j):
            for m in range(i):
                gram[j, i] = gram[j, i] - gram[j, m] * lower[i, m]
            lower[j, i] = gram[j, i] / pivot[i]
        pivot[j] = gram[j, j]
        for i in range(j):
            pivot[j] = pivot[j] - lower[j, i] * gram[j, i]
            load[j] = load[j] - lower[j, i] * load[i]
    weight = {}
    for j in reversed(range(ITERS)):
        weight[j] = load[j] / pivot[j]
        for i in range(j + 1, ITERS):
            weight[j] = weight[j] - lower[i, j] * weight[i]
    for k in range(levels):
        total, left = None, side_ref[k]
        for i in range(ITERS):
            term = weight[i] * basis[i, k]
            total = term if total is None else total + term
            left = left - weight[i] * image[i, k]
        out_ref[0, k] = total
        out_ref[1, k] = left
    for copy in pending:
        copy.wait_send()
    for side, copy in beside:
        pl.when(me != (bands - 1) * side)(copy.wait_send)


def body(mesh, right_side, diag_shift, level_scale):
    levels, rows, n = right_side.shape
    plan = Plan(mesh, levels, rows, n)
    bands, columns, per = plan.bands, plan.columns, plan.per
    field = jax.ShapeDtypeStruct((2, *right_side.shape), F32)
    vmem = pl.BlockSpec(memory_space=pltpu.VMEM)
    dma = pltpu.SemaphoreType.DMA
    block = levels * rows
    tables = plan.tables()
    both = pl.pallas_call(
        functools.partial(kernel, plan),
        out_shape=field,
        in_specs=[pl.BlockSpec(memory_space=pltpu.SMEM)] + [vmem] * (2 + len(tables)),
        out_specs=vmem,
        scratch_shapes=[
            pltpu.VMEM((levels, rows, n), F32),
            pltpu.VMEM((levels, rows, n), F32),
            pltpu.VMEM((ITERS, levels, rows, n), F32),
            pltpu.VMEM((ITERS, levels, rows, n), F32),
            pltpu.VMEM((ITERS, 8, n), F32),
            pltpu.VMEM((plan.blocks * block, per * 2 * LANES), F32),
            pltpu.VMEM((plan.blocks, 8, plan.groups * plan.lanes), F32),
            pltpu.VMEM((plan.latitudes, plan.lanes), F32),
            pltpu.VMEM((ITERS * (ITERS + 1), 1, LANES), F32),
            pltpu.VMEM((ITERS, bands, rows, plan.lanes), F32),
            pltpu.VMEM((ITERS, bands, rows, plan.lanes), F32),
            pltpu.VMEM((ITERS, bands, plan.chunk, LANES), F32),
            pltpu.VMEM((ITERS, bands, plan.chunk, LANES), F32),
            pltpu.VMEM((ITERS, 2, levels, 1, n), F32),
            pltpu.VMEM((ITERS, 2, levels, 1, n), F32),
            pltpu.VMEM((1, LANES), F32),
            pltpu.VMEM((bands, columns, 1, LANES), F32),
            dma((ITERS, bands)), dma((ITERS, bands)), dma((ITERS, bands)), dma((ITERS, bands)),
            dma((ITERS, 2)), dma((ITERS, 2)),
            dma((bands, columns)), dma((bands, columns)),
        ],
        compiler_params=pltpu.CompilerParams(collective_id=0, has_side_effects=True),
    )(level_scale, right_side, diag_shift, *tables)
    return both[0], both[1]


def solution(mesh):
    placed = (P("lev", "lat", None), P("lev", "lat", None), P("lev"))
    return jax.shard_map(
        functools.partial(body, mesh),
        mesh=mesh,
        in_specs=placed,
        out_specs=(P("lev", "lat", None), P("lev", "lat", None)),
        check_vma=False,
    )
```
